32 devices in a mesh: client: 4 (over z), tensor: 4 (over x, core), sdata: 2 (over y).
Axes of the slice: x: 2, y: 2, z: 4, core: 2. Of those that a mesh axis runs over, the one named last changes fastest.
Arguments:
- client_input: bfloat16 [3072, 2048], P(('client', 'sdata')), may hold values from -6 to 6
- client_gain: bfloat16 [4, 2048], P('client'), may hold values from 0.5 to 1.5
- query_weight: bfloat16 [4, 2048, 2048], P('client', None, 'tensor'), as said below
- key_weight: bfloat16 [4, 2048, 512], P('client', None, 'tensor'), as said below
- client_value_weight: bfloat16 [4, 2048, 512], P('client', None, 'tensor'), may hold values from -0.125 to 0.125
- output_weight: bfloat16 [4, 2048, 2048], P('client', None, 'tensor'), may hold values from -0.125 to 0.125
- server_gain: bfloat16 [2, 2048], P('sdata'), may hold values from 0.5 to 1.5
- server_gate: bfloat16 [2, 2048, 4096], P('sdata', None, 'tensor'), may hold values from -0.125 to 0.125
- server_up: bfloat16 [2, 2048, 4096], P('sdata', None, 'tensor'), may hold values from -0.125 to 0.125
- server_down: bfloat16 [2, 4096, 2048], P('sdata', 'tensor'), may hold values from -0.09375 to 0.09375
- upstream: bfloat16 [3072, 2048], P(('client', 'sdata')), may hold values from -6 to 6
- assignment: int32 [4], replicated, may hold values from 0 to 1, as said below
Outputs:
- query_update: bfloat16 [2048, 2048], P(('client', 'sdata'), 'tensor')
- key_update: bfloat16 [2048, 512], P(('client', 'sdata'), 'tensor')
- value_update: bfloat16 [2048, 512], P(('client', 'sdata'), 'tensor')
- output_update: bfloat16 [2048, 2048], P(('client', 'sdata'), 'tensor')
The draws below stay inside these ranges and needn't reach their ends.
Inputs may be any that keep to these rules, and one draw needn't show every extreme that they name: `assignment`: each of the 2 server groups is named by exactly 2 clients. `query_weight`: independent entries with a spread of about 2048 ** -0.5. `key_weight`: entries with a spread of about 2048 ** -0.5 or more.
All inputs are finite; a program needn't handle non-finite values.
Results may differ from the reference program's by a relative error of at most 0.038.
The reference program's roundings to bfloat16 on the way count: a program that leaves them out, or rounds other values in their place, can miss the bound.
Values may be sent and summed in bfloat16 or wider, within the bound.
A program may use at most 128 MiB of HBM per device.

```python
import math
import jax
import jax.numpy as jnp
from jax import lax

MODEL_WIDTH = 2048
HEAD_DIM = 64
FF = 4096
LEN = 384
CLIENT_TOTAL = 4
GROUPS = 2
TOKENS = 3072
QUERY_FEATURES = 2048
KEY_FEATURES = 512


def weights_pair(key):
    scaling_factor = MODEL_WIDTH ** (-0.5)
    query_matrix = jnp.clip(jax.random.normal(jax.random.fold_in(key, 11), (CLIENT_TOTAL, MODEL_WIDTH, QUERY_FEATURES), jnp.float32), -4.0, 4.0) * scaling_factor
    client_key_matrix = jnp.clip(jax.random.normal(jax.random.fold_in(key, 12), (CLIENT_TOTAL, MODEL_WIDTH, KEY_FEATURES), jnp.float32), -4.0, 4.0) * scaling_factor
    return (query_matrix, client_key_matrix)


def draw_query_weight(key, part):
    return weights_pair(key)[0].astype(jnp.bfloat16)


def draw_key_weight(key, part):
    return weights_pair(key)[1].astype(jnp.bfloat16)


def draw_assignment(key, part):
    scores = jax.random.randint(jax.random.fold_in(key, 4099), (CLIENT_TOTAL,), 0, 1 << 20) * CLIENT_TOTAL + jnp.arange(CLIENT_TOTAL)
    order = jnp.argsort(scores, stable=True)
    return (order % GROUPS).astype(jnp.int32)


def strengthened(entries, own_key, source, target, shards_of, factor):
    def block_of(axis_at):
        return (jnp.arange(entries.shape[axis_at]) // (entries.shape[axis_at] // shards_of)).reshape((-1,) + (1,) * (entries.ndim - 1 - axis_at))

    near = jax.random.permutation(own_key, shards_of)[block_of(target)]
    far = (block_of(target) + shards_of // 2) % shards_of
    return jnp.where((block_of(source) == near) | (block_of(source) == far), factor * entries, entries)


def level_of(key, shape, pieces, least, largest):
    def one(dim, parts):
        steps = jax.random.uniform(jax.random.fold_in(jax.random.fold_in(key, 6), dim), (parts,), jnp.float32, least / len(pieces), largest / len(pieces))
        return jnp.repeat(jnp.exp(steps), shape[dim] // parts).reshape((-1,) + (1,) * (len(shape) - dim - 1))

    level = one(*pieces[0])
    for cut in pieces[1:]:
        level = level * one(*cut)
    return level


def noise(rng, shape, deviation, most, pieces=(), kind=jnp.bfloat16):
    array = jax.random.normal(rng, shape, jnp.float32) * deviation
    if len(pieces) > 0:
        array = level_of(rng, shape, pieces, -0.22, 0.18) * array
    return jnp.clip(array, min=-most, max=most).astype(kind)


def noise_with(stream_key, shape, scale, limit, pieces, heavy, held_as=jnp.bfloat16):
    array = scale * jax.random.normal(stream_key, shape, jnp.float32)
    if pieces:
        array = array * level_of(stream_key, shape, pieces, -0.22, 0.18)
    return jnp.clip(strengthened(array, jax.random.fold_in(stream_key, 3), *heavy), -limit, limit).astype(held_as)


def setup_inputs(seed: int = 0) -> dict:
    streams_of = jax.random.split(jax.random.key(seed), 13)
    return {
        "client_input": noise_with(streams_of[0], (TOKENS, MODEL_WIDTH), 1.0, 6.0, ((0, 8),), (0, 1, 8, 2.0)),
        "client_gain": jnp.clip(1.0 + 0.1 * jax.random.normal(streams_of[1], (CLIENT_TOTAL, MODEL_WIDTH), jnp.float32), 0.5, 1.5).astype(jnp.bfloat16),
        "query_weight": draw_query_weight(jax.random.fold_in(streams_of[12], 71), 0),
        "key_weight": draw_key_weight(jax.random.fold_in(streams_of[12], 71), 0),
        "client_value_weight": noise(streams_of[4], (CLIENT_TOTAL, MODEL_WIDTH, KEY_FEATURES), MODEL_WIDTH ** -0.5, 0.125, ((0, 4), (2, 4))),
        "output_weight": noise(streams_of[5], (CLIENT_TOTAL, MODEL_WIDTH, QUERY_FEATURES), QUERY_FEATURES ** -0.5, 0.125, ((0, 4), (2, 4))),
        "server_gain": jnp.clip(1.0 + 0.1 * jax.random.normal(streams_of[6], (GROUPS, MODEL_WIDTH), jnp.float32), 0.5, 1.5).astype(jnp.bfloat16),
        "server_gate": noise(streams_of[7], (GROUPS, MODEL_WIDTH, FF), MODEL_WIDTH ** -0.5, 0.125, ((0, 2), (2, 4))),
        "server_up": noise(streams_of[8], (GROUPS, MODEL_WIDTH, FF), MODEL_WIDTH ** -0.5, 0.125, ((0, 2), (2, 4))),
        "server_down": noise(streams_of[9], (GROUPS, FF, MODEL_WIDTH), FF ** -0.5, 0.09375, ((0, 2), (1, 4))),
        "upstream": noise(streams_of[10], (TOKENS, MODEL_WIDTH), 1.0, 6.0, ((0, 8),)),
        "assignment": draw_assignment(jax.random.fold_in(streams_of[12], 71), 0),
    }


def rotary_tables(length):
    halfway = HEAD_DIM // 2
    positions = jnp.arange(length).astype(jnp.float32)
    exponents = jnp.arange(halfway).astype(jnp.float32) * (2.0 / HEAD_DIM)
    frequencies = jnp.exp(-math.log(500000.0) * exponents)
    angles = positions[:, None] * frequencies[None, :]
    cosine_table = jnp.concatenate([jnp.cos(angles), jnp.cos(angles)], 1)
    sine_table = jnp.concatenate([jnp.sin(angles), jnp.sin(angles)], 1)
    return (cosine_table, sine_table)

def rotary(heads_in, cosine_table, sine_table):
    halfway = heads_in.shape[-1] // 2
    turned = jnp.concatenate([-heads_in[..., halfway:], heads_in[..., :halfway]], -1)
    return heads_in * cosine_table[:, None, :] + turned * sine_table[:, None, :]

def normalize(rows_in, gain):
    rows_float = rows_in.astype(jnp.float32)
    inv_rms = lax.rsqrt(lax.optimization_barrier(jnp.mean(rows_float * rows_float, -1, keepdims=True)) + 1e-05)
    return (rows_float * inv_rms * gain.astype(jnp.float32)).astype(jnp.bfloat16)

def attention_part(normed, query_matrix, client_key_matrix, value_matrix, output_matrix):
    length = normed.shape[0]
    query_count = query_matrix.shape[1] // HEAD_DIM
    shared_count = client_key_matrix.shape[1] // HEAD_DIM
    group_size = query_count // shared_count
    cosine_table, sine_table = rotary_tables(length)
    queries = jnp.dot(normed, query_matrix, preferred_element_type=jnp.float32).reshape(length, query_count, HEAD_DIM)
    queries = rotary(queries, cosine_table, sine_table).astype(jnp.bfloat16).reshape(length, shared_count, group_size, HEAD_DIM)
    key_heads = jnp.dot(normed, client_key_matrix, preferred_element_type=jnp.float32).reshape(length, shared_count, HEAD_DIM)
    key_heads = rotary(key_heads, cosine_table, sine_table).astype(jnp.bfloat16)
    value_heads = jnp.dot(normed, value_matrix, preferred_element_type=jnp.float32).astype(jnp.bfloat16).reshape(length, shared_count, HEAD_DIM)
    scores = jnp.einsum('qgrd,kgd->grqk', queries.astype(jnp.float32), key_heads.astype(jnp.float32)) * HEAD_DIM ** (-0.5)
    row_ids = lax.broadcasted_iota(jnp.int32, (length, length), 0)
    col_ids = lax.broadcasted_iota(jnp.int32, (length, length), 1)
    scores = jnp.where(col_ids <= row_ids, scores, -1e+30)
    highest = lax.stop_gradient(lax.optimization_barrier(jnp.max(scores, -1, keepdims=True)))
    exponent = jnp.exp(scores - highest)
    weights = (exponent / lax.optimization_barrier(jnp.sum(exponent, -1, keepdims=True))).astype(jnp.bfloat16)
    context = jnp.einsum('grqk,kgd->qgrd', weights.astype(jnp.float32), value_heads.astype(jnp.float32))
    context = context.astype(jnp.bfloat16).reshape(length, query_count * HEAD_DIM)
    return lax.dot_general(context, output_matrix, (((1,), (1,)), ((), ())), preferred_element_type=jnp.float32)

def server_pull(rows_in, upstream_rows, gain, gate_matrix, up_matrix, down_matrix):
    rows_float = rows_in.astype(jnp.float32)
    inv_rms = lax.rsqrt(lax.optimization_barrier(jnp.mean(rows_float * rows_float, -1, keepdims=True)) + 1e-05)
    gain_float = gain.astype(jnp.float32)
    server_normed = (rows_float * inv_rms * gain_float).astype(jnp.bfloat16)
    gate_value = jnp.dot(server_normed, gate_matrix, preferred_element_type=jnp.float32)
    up_value = jnp.dot(server_normed, up_matrix, preferred_element_type=jnp.float32)
    pulled = lax.dot_general(upstream_rows, down_matrix, (((1,), (1,)), ((), ())), preferred_element_type=jnp.float32)
    sigmoid_gate = jax.nn.sigmoid(gate_value)
    gate_grad = (pulled * up_value * sigmoid_gate * (1.0 + gate_value * (1.0 - sigmoid_gate))).astype(jnp.bfloat16)
    up_grad = (pulled * gate_value * sigmoid_gate).astype(jnp.bfloat16)
    normed_grad = lax.dot_general(gate_grad, gate_matrix, (((1,), (1,)), ((), ())), preferred_element_type=jnp.float32)
    normed_grad = normed_grad + lax.dot_general(up_grad, up_matrix, (((1,), (1,)), ((), ())), preferred_element_type=jnp.float32)
    weighted = normed_grad * gain_float
    return inv_rms * weighted - rows_float * inv_rms ** 3 * lax.optimization_barrier(jnp.mean(weighted * rows_float, -1, keepdims=True))

def reference(client_input, client_gain, query_weight, key_weight, client_value_weight, output_weight, server_gain, server_gate, server_up, server_down, upstream, assignment):
    sequences = client_input.reshape(CLIENT_TOTAL * GROUPS, LEN, MODEL_WIDTH)
    upstream_seqs = upstream.reshape(CLIENT_TOTAL * GROUPS, LEN, MODEL_WIDTH)

    def one_sequence(totals, index_seq):
        owner_client = index_seq // GROUPS
        group_index = assignment[owner_client]
        rows_in = sequences[index_seq]
        upstream_rows = upstream_seqs[index_seq]
        normed = normalize(rows_in, client_gain[owner_client])

        def client_part(query_matrix, client_key_matrix, value_matrix, output_matrix):
            return attention_part(normed, query_matrix, client_key_matrix, value_matrix, output_matrix)
        attended, pullback = jax.vjp(client_part, query_weight[owner_client], key_weight[owner_client], client_value_weight[owner_client], output_weight[owner_client])
        cut_input = (rows_in.astype(jnp.float32) + attended).astype(jnp.bfloat16)
        pulled = server_pull(cut_input, upstream_rows, server_gain[group_index], server_gate[group_index], server_up[group_index], server_down[group_index])
        cut_grad = (upstream_rows.astype(jnp.float32) + pulled).astype(jnp.bfloat16)
        gradients = pullback(cut_grad.astype(jnp.float32))
        updated = tuple((total + grad_item.astype(jnp.bfloat16).astype(jnp.float32) for total, grad_item in zip(totals, gradients)))
        return (updated, None)
    start_offsets = (jnp.zeros((MODEL_WIDTH, QUERY_FEATURES), jnp.float32), jnp.zeros((MODEL_WIDTH, KEY_FEATURES), jnp.float32), jnp.zeros((MODEL_WIDTH, KEY_FEATURES), jnp.float32), jnp.zeros((MODEL_WIDTH, QUERY_FEATURES), jnp.float32))
    totals, unused = lax.scan(one_sequence, start_offsets, jnp.arange(CLIENT_TOTAL * GROUPS).astype(jnp.int32))
    query_total, key_total, value_total, output_total = totals
    return ((query_total / CLIENT_TOTAL).astype(jnp.bfloat16), (key_total / CLIENT_TOTAL).astype(jnp.bfloat16), (value_total / CLIENT_TOTAL).astype(jnp.bfloat16), (output_total / CLIENT_TOTAL).astype(jnp.bfloat16))
```

```python
from functools import partial
import math

import jax
import jax.numpy as jnp
from jax import lax
from jax.experimental import pallas as pl
from jax.experimental.pallas import tpu as pltpu
from jax.sharding import PartitionSpec as P

HEAD_DIM = 64
MESH = pl.DeviceIdType.MESH
CORES = 2
BF16 = jnp.bfloat16
F32 = jnp.float32


def rotary_tables(length):
    halfway = HEAD_DIM // 2
    positions = jnp.arange(length).astype(jnp.float32)
    exponents = jnp.arange(halfway).astype(jnp.float32) * (2.0 / HEAD_DIM)
    frequencies = jnp.exp(-math.log(500000.0) * exponents)
    angles = positions[:, None] * frequencies[None, :]
    cosine_table = jnp.concatenate([jnp.cos(angles), jnp.cos(angles)], 1)
    sine_table = jnp.concatenate([jnp.sin(angles), jnp.sin(angles)], 1)
    return (cosine_table, sine_table)


def rotary(heads_in, cosine_table, sine_table):
    halfway = heads_in.shape[-1] // 2
    turned = jnp.concatenate([-heads_in[..., halfway:], heads_in[..., :halfway]], -1)
    return heads_in * cosine_table[:, None, :] + turned * sine_table[:, None, :]


def normalize(rows_in, gain):
    rows_float = rows_in.astype(jnp.float32)
    inv_rms = lax.rsqrt(jnp.mean(rows_float * rows_float, -1, keepdims=True) + 1e-05)
    return (rows_float * inv_rms * gain.astype(jnp.float32)).astype(jnp.bfloat16)


def attention_part(normed, query_matrix, client_key_matrix, value_matrix, output_matrix):
    length = normed.shape[0]
    query_count = query_matrix.shape[1] // HEAD_DIM
    shared_count = client_key_matrix.shape[1] // HEAD_DIM
    group_size = query_count // shared_count
    cosine_table, sine_table = rotary_tables(length)
    queries = jnp.dot(normed, query_matrix, preferred_element_type=jnp.float32).reshape(
        length, query_count, HEAD_DIM
    )
    queries = (
        rotary(queries, cosine_table, sine_table)
        .astype(jnp.bfloat16)
        .reshape(length, shared_count, group_size, HEAD_DIM)
    )
    key_heads = jnp.dot(normed, client_key_matrix, preferred_element_type=jnp.float32).reshape(
        length, shared_count, HEAD_DIM
    )
    key_heads = rotary(key_heads, cosine_table, sine_table).astype(jnp.bfloat16)
    value_heads = (
        jnp.dot(normed, value_matrix, preferred_element_type=jnp.float32)
        .astype(jnp.bfloat16)
        .reshape(length, shared_count, HEAD_DIM)
    )
    scores = jnp.einsum(
        "qgrd,kgd->grqk", queries.astype(jnp.float32), key_heads.astype(jnp.float32)
    ) * HEAD_DIM ** (-0.5)
    row_ids = lax.broadcasted_iota(jnp.int32, (length, length), 0)
    col_ids = lax.broadcasted_iota(jnp.int32, (length, length), 1)
    scores = jnp.where(col_ids <= row_ids, scores, -1e30)
    highest = lax.stop_gradient(jnp.max(scores, -1, keepdims=True))
    exponent = jnp.exp(scores - highest)
    weights = (exponent / jnp.sum(exponent, -1, keepdims=True)).astype(jnp.bfloat16)
    context = jnp.einsum(
        "grqk,kgd->qgrd", weights.astype(jnp.float32), value_heads.astype(jnp.float32)
    )
    context = context.astype(jnp.bfloat16).reshape(length, query_count * HEAD_DIM)
    return lax.dot_general(
        context, output_matrix, (((1,), (1,)), ((), ())), preferred_element_type=jnp.float32
    )


def server_pull(rows_in, upstream_rows, gain, gate_matrix, up_matrix, down_matrix):
    rows_float = rows_in.astype(jnp.float32)
    inv_rms = lax.rsqrt(jnp.mean(rows_float * rows_float, -1, keepdims=True) + 1e-05)
    gain_float = gain.astype(jnp.float32)
    server_normed = (rows_float * inv_rms * gain_float).astype(jnp.bfloat16)
    gate_value = jnp.dot(server_normed, gate_matrix, preferred_element_type=jnp.float32)
    up_value = jnp.dot(server_normed, up_matrix, preferred_element_type=jnp.float32)
    pulled = lax.dot_general(
        upstream_rows, down_matrix, (((1,), (1,)), ((), ())), preferred_element_type=jnp.float32
    )
    sigmoid_gate = jax.nn.sigmoid(gate_value)
    gate_grad = (
        pulled * up_value * sigmoid_gate * (1.0 + gate_value * (1.0 - sigmoid_gate))
    ).astype(jnp.bfloat16)
    up_grad = (pulled * gate_value * sigmoid_gate).astype(jnp.bfloat16)
    normed_grad = lax.dot_general(
        gate_grad, gate_matrix, (((1,), (1,)), ((), ())), preferred_element_type=jnp.float32
    )
    normed_grad = normed_grad + lax.dot_general(
        up_grad, up_matrix, (((1,), (1,)), ((), ())), preferred_element_type=jnp.float32
    )
    weighted = normed_grad * gain_float
    return inv_rms * weighted - rows_float * inv_rms**3 * jnp.mean(
        weighted * rows_float, -1, keepdims=True
    )


def greet(others):
    barrier = pltpu.get_barrier_semaphore()
    for other in others:
        pl.semaphore_signal(barrier, inc=1, device_id=other, device_id_type=MESH)
    pl.semaphore_wait(barrier, len(others))


def send(source, target, send_sem, recv_sem, device):
    copy = pltpu.make_async_remote_copy(
        src_ref=source,
        dst_ref=target,
        send_sem=send_sem,
        recv_sem=recv_sem,
        device_id=device,
        device_id_type=MESH,
    )
    copy.start()
    return copy


def place():
    tensor_at = lax.axis_index("tensor")
    return tensor_at // CORES, lax.rem(tensor_at, CORES)


def turned(index, step, count):
    return lax.rem(index + step, count)


def columns_of(chip, core, width):
    return pl.ds(pl.multiple_of((chip * CORES + core) * width, width), width)


def partners(chips, client_count, group_count):
    chip, core = place()
    client, group = lax.axis_index("client"), lax.axis_index("sdata")
    others = [{"tensor": chip * CORES + 1 - core}]
    others += [{"tensor": turned(chip, k, chips) * CORES + core} for k in range(1, chips)]
    others += [{"client": turned(client, k, client_count)} for k in range(1, client_count)]
    others += [{"sdata": turned(group, k, group_count)} for k in range(1, group_count)]
    return others


class ShareSum:
    def __init__(self, part, pair, relay, landed, sems, chunks, chips):
        self.part, self.pair, self.relay, self.landed = part, pair, relay, landed
        self.pair_send, self.pair_recv, self.chip_send, self.chip_recv = sems
        self.chips, self.width = chips, part.shape[-1] // (CORES * chips)
        self.chip, self.core = place()
        self.copies = []
        self.pair_copies = {}
        self.chip_copies = {}
        for n, q in enumerate(chunks):
            for k in list(range(1, chips)) + [0]:
                to = turned(self.chip, k, chips)
                copy = send(
                    part.at[q, :, columns_of(to, 1 - self.core, self.width)],
                    pair.at[k, q],
                    self.pair_send.at[k, n],
                    self.pair_recv.at[k, n],
                    {"tensor": self.chip * CORES + 1 - self.core},
                )
                self.pair_copies[k, n] = copy
        for n, q in enumerate(chunks):
            for k in range(1, chips):
                to = turned(self.chip, k, chips)
                self.pair_copies[k, n].wait_recv()
                relay[k, q] = (
                    part[q, :, columns_of(to, self.core, self.width)].astype(F32)
                    + pair[k, q].astype(F32)
                ).astype(BF16)
                self.chip_copies[k, n] = send(
                    relay.at[k, q],
                    landed.at[k, q],
                    self.chip_send.at[k, n],
                    self.chip_recv.at[k, n],
                    {"tensor": to * CORES + self.core},
                )

    def get(self, n, q):
        self.pair_copies[0, n].wait_recv()
        total = self.part[q, :, columns_of(self.chip, self.core, self.width)].astype(
            F32
        ) + self.pair[0, q].astype(F32)
        for k in range(1, self.chips):
            self.chip_copies[k, n].wait_recv()
            total = total + self.landed[k, q].astype(F32)
        return total

    def finish(self):
        for copy in list(self.pair_copies.values()) + list(self.chip_copies.values()):
            copy.wait_send()


class Widen:
    def __init__(self, out, sems, chips):
        self.out, self.chips = out, chips
        self.chip_send, self.chip_recv, self.pair_send, self.pair_recv = sems
        self.chip, self.core = place()
        self.width = out.shape[-1] // (CORES * chips)
        self.started, self.forwarded, self.chip_copies = [], [], {}

    def pair_copy(self, source, k, n, q):
        cols = columns_of(turned(self.chip, self.chips - k, self.chips), self.core, self.width)
        self.forwarded.append(
            send(
                source,
                self.out.at[q, :, cols],
                self.pair_send.at[k, n],
                self.pair_recv.at[k, n],
                {"tensor": self.chip * CORES + 1 - self.core},
            )
        )

    def start(self, source, n, q):
        cols = columns_of(self.chip, self.core, self.width)
        for k in range(1, self.chips):
            self.chip_copies[k, n] = send(
                source,
                self.out.at[q, :, cols],
                self.chip_send.at[k, n],
                self.chip_recv.at[k, n],
                {"tensor": turned(self.chip, k, self.chips) * CORES + self.core},
            )
        self.pair_copy(source, 0, n, q)
        self.out[q, :, cols] = source[...]

    def forward(self, n, q):
        for k in range(1, self.chips):
            self.chip_copies[k, n].wait_recv()
            cols = columns_of(turned(self.chip, self.chips - k, self.chips), self.core, self.width)
            self.pair_copy(self.out.at[q, :, cols], k, n, q)

    def finish(self):
        for copy in self.forwarded:
            copy.wait_recv()
        for copy in self.forwarded + list(self.chip_copies.values()):
            copy.wait_send()


def out_kernel(
    chips, client_count, group_count,
    order, part, inputs, upstream,
    cut_out, up_out, up_own,
    pair, relay, landed, cut_from, cut_at, up_at, cut_put, up_put, cut_own,
    tp_sems, z_sems, y_sems, wide_sems,
):
    client, group = lax.axis_index("client"), lax.axis_index("sdata")
    chip, core = place()
    share = client_count // group_count
    width = part.shape[-1] // (CORES * chips)
    cols = columns_of(chip, core, width)
    greet(partners(chips, client_count, group_count))
    steps = list(range(1, client_count)) + [0]
    targets = [turned(client, k, client_count) for k in steps]
    up_z = []
    sums = ShareSum(part, pair, relay, landed, [tp_sems.at[i] for i in range(4)], targets, chips)
    for k in range(1, client_count):
        to = turned(client, k, client_count)
        up_z.append(
            send(
                upstream.at[to, :, cols], up_at.at[client],
                z_sems.at[0, k], z_sems.at[1, k], {"client": to},
            )
        )
    up_at[client] = upstream[client, :, cols]
    cut_z = []
    for n, (k, to) in enumerate(zip(steps, targets)):
        block = (sums.get(n, to) + inputs[to, :, cols].astype(F32)).astype(BF16)
        if k == 0:
            cut_at[client] = block
        else:
            cut_from[k] = block
            cut_z.append(
                send(
                    cut_from.at[k], cut_at.at[client],
                    z_sems.at[2, k], z_sems.at[3, k], {"client": to},
                )
            )
    widens = [
        Widen(up_out, [wide_sems.at[i] for i in range(4)], chips),
        Widen(cut_out, [wide_sems.at[i] for i in range(4, 8)], chips),
    ]
    rounds = []
    for which, (z_copies, at, put, own) in enumerate(
        ((up_z, up_at, up_put, up_own), (cut_z, cut_at, cut_put, cut_own))
    ):
        for copy in z_copies:
            copy.wait_recv()
        y_copies = []
        for d in range(1, group_count):
            to = turned(group, d, group_count)
            for i in range(share):
                put[d, i] = at[order[to * share + i]]
                y_copies.append(
                    (
                        send(
                            put.at[d, i], own.at[group * share + i],
                            y_sems.at[2 * which, d, i], y_sems.at[2 * which + 1, d, i],
                            {"sdata": to},
                        ),
                        turned(group, group_count - d, group_count) * share + i,
                    )
                )
        n = 0
        for i in range(share):
            q = group * share + i
            own[q] = at[order[group * share + i]]
            widens[which].start(own.at[q], n, q)
            rounds.append((which, n, q))
            n += 1
        for copy, q in y_copies:
            copy.wait_recv()
            widens[which].start(own.at[q], n, q)
            rounds.append((which, n, q))
            n += 1
        for copy, q in y_copies:
            copy.wait_send()
    for which, n, q in rounds:
        widens[which].forward(n, q)
    for widen in widens:
        widen.finish()
    sums.finish()
    for copy in up_z + cut_z:
        copy.wait_send()


def back_kernel(
    chips, client_count, group_count,
    inverse, part, up_own,
    grad_out,
    pair, relay, landed, y_from, y_at, z_from, own,
    tp_sems, y_sems, z_sems, wide_sems,
):
    client, group = lax.axis_index("client"), lax.axis_index("sdata")
    share = client_count // group_count
    greet(partners(chips, client_count, group_count))
    steps = [(d, i) for d in list(range(1, group_count)) + [0] for i in range(share)]
    chunks = [turned(group, d, group_count) * share + i for d, i in steps]
    sums = ShareSum(part, pair, relay, landed, [tp_sems.at[i] for i in range(4)], chunks, chips)
    y_copies = []
    for n, ((d, i), q) in enumerate(zip(steps, chunks)):
        block = (sums.get(n, q) + up_own[q].astype(F32)).astype(BF16)
        if d == 0:
            y_at[group * share + i] = block
        else:
            y_from[d, i] = block
            y_copies.append(
                send(
                    y_from.at[d, i], y_at.at[group * share + i],
                    y_sems.at[0, d, i], y_sems.at[1, d, i],
                    {"sdata": turned(group, d, group_count)},
                )
            )
    for copy in y_copies:
        copy.wait_recv()
    widen = Widen(grad_out, [wide_sems.at[i] for i in range(4)], chips)
    z_copies = []
    for k in list(range(1, client_count)):
        to = turned(client, k, client_count)
        z_from[k] = y_at[inverse[to]]
        z_copies.append(
            send(
                z_from.at[k], own.at[client], z_sems.at[0, k], z_sems.at[1, k], {"client": to}
            )
        )
    own[client] = y_at[inverse[client]]
    widen.start(own.at[client], 0, client)
    for k, copy in enumerate(z_copies, 1):
        copy.wait_recv()
        source = turned(client, client_count - k, client_count)
        widen.start(own.at[source], k, source)
    for k in range(client_count):
        widen.forward(k, turned(client, client_count - k, client_count))
    widen.finish()
    sums.finish()
    for copy in y_copies + z_copies:
        copy.wait_send()


def average_kernel(client_count, group_count, count, *refs):
    grads, outs = refs[:count], refs[count : 2 * count]
    y_at, z_from, z_at = (refs[(2 + i) * count : (3 + i) * count] for i in range(3))
    y_sems, z_sems = refs[5 * count :]
    client, group = lax.axis_index("client"), lax.axis_index("sdata")
    others = [{"client": turned(client, k, client_count)} for k in range(1, client_count)]
    others += [{"sdata": turned(group, k, group_count)} for k in range(1, group_count)]
    greet(others)
    middle = client_count // 2
    steps = [(middle + k) % client_count for k in range(client_count)]
    steps = [k for k in steps if k != 0] + [0]
    y_copies = {}
    for k in steps:
        to = turned(client, k, client_count)
        for a in range(count):
            for d in range(1, group_count):
                y_copies[k, a, d] = send(
                    grads[a].at[to, turned(group, d, group_count)], y_at[a].at[d, to],
                    y_sems.at[0, a, d, k], y_sems.at[1, a, d, k],
                    {"sdata": turned(group, d, group_count)},
                )
    z_copies = []
    rows = outs[0].shape[0]
    block = next(b for b in (64, 32, 16, rows) if rows % b == 0)
    for k in steps:
        to = turned(client, k, client_count)
        for a in range(count):
            for d in range(1, group_count):
                y_copies[k, a, d].wait_recv()
            for r in range(0, rows, block):
                at = pl.ds(r, block)
                total = grads[a][to, group, at, :].astype(F32)
                for d in range(1, group_count):
                    total = total + y_at[a][d, to, at, :].astype(F32)
                z_from[a][k, at, :] = total.astype(BF16)
            if k != 0:
                z_copies.append(
                    send(
                        z_from[a].at[k], z_at[a].at[k],
                        z_sems.at[0, a, k], z_sems.at[1, a, k], {"client": to},
                    )
                )
    for copy in z_copies:
        copy.wait_recv()
    for a in range(count):
        for r in range(0, rows, block):
            at = pl.ds(r, block)
            total = z_from[a][0, at, :].astype(F32)
            for k in range(1, client_count):
                total = total + z_at[a][k, at, :].astype(F32)
            outs[a][at, :] = (total * (1.0 / client_count)).astype(BF16)
    for copy in list(y_copies.values()) + z_copies:
        copy.wait_send()


VMEM_SPEC = pl.BlockSpec(memory_space=pltpu.VMEM)
SMEM_SPEC = pl.BlockSpec(memory_space=pltpu.SMEM)


def params(number):
    return pltpu.CompilerParams(
        collective_id=number, has_side_effects=True, vmem_limit_bytes=48 * 2**20
    )


def axis_counts():
    return lax.axis_size("tensor") // CORES, lax.axis_size("client"), lax.axis_size("sdata")


def relay_out(order, attended, rows_in, upstream):
    chips, client_count, group_count = axis_counts()
    length, breadth = rows_in.shape
    chunk, width = length // client_count, breadth // (CORES * chips)
    share = client_count // group_count
    full = (client_count, chunk, breadth)
    own = (client_count, chunk, width)
    dma = pltpu.SemaphoreType.DMA
    vmem = lambda shape: pltpu.VMEM(shape, BF16)
    cut, up, up_own = pl.pallas_call(
        partial(out_kernel, chips, client_count, group_count),
        out_shape=(
            jax.ShapeDtypeStruct(full, BF16),
            jax.ShapeDtypeStruct(full, BF16),
            jax.ShapeDtypeStruct(own, BF16),
        ),
        in_specs=[SMEM_SPEC, VMEM_SPEC, VMEM_SPEC, VMEM_SPEC],
        out_specs=(VMEM_SPEC,) * 3,
        scratch_shapes=[
            vmem((chips,) + own), vmem((chips,) + own), vmem((chips,) + own),
            vmem(own), vmem(own), vmem(own),
            vmem((group_count, share, chunk, width)), vmem((group_count, share, chunk, width)),
            vmem(own),
            dma((4, chips, client_count)), dma((4, client_count)),
            dma((4, group_count, share)), dma((8, chips, client_count)),
        ],
        compiler_params=params(1),
        name="relay_out",
    )(order, attended.reshape(full), rows_in.reshape(full), upstream.reshape(full))
    return cut.reshape(length, breadth), up.reshape(length, breadth), up_own


def relay_back(inverse, pulled, up_own):
    chips, client_count, group_count = axis_counts()
    length, breadth = pulled.shape
    chunk, width = length // client_count, breadth // (CORES * chips)
    share = client_count // group_count
    full = (client_count, chunk, breadth)
    own = (client_count, chunk, width)
    dma = pltpu.SemaphoreType.DMA
    vmem = lambda shape: pltpu.VMEM(shape, BF16)
    grad = pl.pallas_call(
        partial(back_kernel, chips, client_count, group_count),
        out_shape=jax.ShapeDtypeStruct(full, BF16),
        in_specs=[SMEM_SPEC, VMEM_SPEC, VMEM_SPEC],
        out_specs=VMEM_SPEC,
        scratch_shapes=[
            vmem((chips,) + own), vmem((chips,) + own), vmem((chips,) + own),
            vmem((group_count, share, chunk, width)), vmem(own), vmem(own), vmem(own),
            dma((4, chips, client_count)), dma((2, group_count, share)),
            dma((2, client_count)), dma((4, chips, client_count)),
        ],
        compiler_params=params(2),
        name="relay_back",
    )(inverse, pulled.reshape(full), up_own)
    return grad.reshape(length, breadth)


def average(grads):
    unused, client_count, group_count = axis_counts()
    count = len(grads)
    rows = grads[0].shape[0] // (client_count * group_count)
    widths = [grad.shape[1] for grad in grads]
    dma = pltpu.SemaphoreType.DMA
    return pl.pallas_call(
        partial(average_kernel, client_count, group_count, count),
        out_shape=tuple(jax.ShapeDtypeStruct((rows, width), BF16) for width in widths),
        in_specs=[VMEM_SPEC] * count,
        out_specs=(VMEM_SPEC,) * count,
        scratch_shapes=[pltpu.VMEM((group_count, client_count, rows, w), BF16) for w in widths]
        + [pltpu.VMEM((client_count, rows, w), BF16) for w in widths]
        + [pltpu.VMEM((client_count, rows, w), BF16) for w in widths]
        + [dma((2, count, group_count, client_count)), dma((2, count, client_count))],
        compiler_params=params(3),
        name="average",
    )(*[grad.reshape(client_count, group_count, rows, grad.shape[1]) for grad in grads])


def local(
    client_input,
    client_gain,
    query_weight,
    key_weight,
    client_value_weight,
    output_weight,
    server_gain,
    server_gate,
    server_up,
    server_down,
    upstream,
    assignment,
):
    client_count = lax.axis_size("client")
    normed = normalize(client_input, client_gain[0])
    attended, pullback = jax.vjp(
        partial(attention_part, normed),
        query_weight[0],
        key_weight[0],
        client_value_weight[0],
        output_weight[0],
    )
    ids = jnp.arange(client_count).astype(jnp.int32)
    ahead = (assignment[None, :] < assignment[:, None]) | (
        (assignment[None, :] == assignment[:, None]) & (ids[None, :] < ids[:, None])
    )
    inverse = jnp.sum(ahead.astype(jnp.int32), 1)
    group_order = jnp.sum(jnp.where(inverse[None, :] == ids[:, None], ids[None, :], 0), 1)
    cut_rows, up_rows, up_own = relay_out(
        group_order, attended.astype(BF16), client_input, upstream
    )
    pulled = server_pull(
        cut_rows, up_rows, server_gain[0], server_gate[0], server_up[0], server_down[0]
    )
    arriving_grad = relay_back(inverse, pulled.astype(BF16), up_own)
    query_grad, key_grad, value_grad, output_grad = pullback(arriving_grad.astype(jnp.float32))
    output_update, query_update, key_update, value_update = average(
        [output_grad, query_grad, key_grad, value_grad]
    )
    return (query_update, key_update, value_update, output_update)


def solution(mesh):
    placed = (
        P(("client", "sdata"), None),
        P("client", None),
        P("client", None, "tensor"),
        P("client", None, "tensor"),
        P("client", None, "tensor"),
        P("client", None, "tensor"),
        P("sdata", None),
        P("sdata", None, "tensor"),
        P("sdata", None, "tensor"),
        P("sdata", "tensor", None),
        P(("client", "sdata"), None),
        P(),
    )
    return jax.shard_map(
        local,
        mesh=mesh,
        in_specs=placed,
        out_specs=(
            P(("client", "sdata"), "tensor"),
            P(("client", "sdata"), "tensor"),
            P(("client", "sdata"), "tensor"),
            P(("client", "sdata"), "tensor"),
        ),
        check_vma=False,
    )
```

```python
from functools import partial
import math

import jax
import jax.numpy as jnp
from jax import lax
from jax.experimental import pallas as pl
from jax.experimental.pallas import tpu as pltpu
from jax.sharding import PartitionSpec as P

HEAD_DIM = 64
MESH = pl.DeviceIdType.MESH
CORES = 2
BF16 = jnp.bfloat16
F32 = jnp.float32


def rotary_tables(length):
    halfway = HEAD_DIM // 2
    positions = jnp.arange(length).astype(jnp.float32)
    exponents = jnp.arange(halfway).astype(jnp.float32) * (2.0 / HEAD_DIM)
    frequencies = jnp.exp(-math.log(500000.0) * exponents)
    angles = positions[:, None] * frequencies[None, :]
    cosine_table = jnp.concatenate([jnp.cos(angles), jnp.cos(angles)], 1)
    sine_table = jnp.concatenate([jnp.sin(angles), jnp.sin(angles)], 1)
    return (cosine_table, sine_table)


def rotary(heads_in, cosine_table, sine_table):
    halfway = heads_in.shape[-1] // 2
    turned = jnp.concatenate([-heads_in[..., halfway:], heads_in[..., :halfway]], -1)
    return heads_in * cosine_table[:, None, :] + turned * sine_table[:, None, :]


def normalize(rows_in, gain):
    rows_float = rows_in.astype(jnp.float32)
    inv_rms = lax.rsqrt(jnp.mean(rows_float * rows_float, -1, keepdims=True) + 1e-05)
    return (rows_float * inv_rms * gain.astype(jnp.float32)).astype(jnp.bfloat16)


def attention_part(normed, query_matrix, client_key_matrix, value_matrix, output_matrix):
    length = normed.shape[0]
    query_count = query_matrix.shape[1] // HEAD_DIM
    shared_count = client_key_matrix.shape[1] // HEAD_DIM
    group_size = query_count // shared_count
    cosine_table, sine_table = rotary_tables(length)
    queries = jnp.dot(normed, query_matrix, preferred_element_type=jnp.float32).reshape(
        length, query_count, HEAD_DIM
    )
    queries = (
        rotary(queries, cosine_table, sine_table)
        .astype(jnp.bfloat16)
        .reshape(length, shared_count, group_size, HEAD_DIM)
    )
    key_heads = jnp.dot(normed, client_key_matrix, preferred_element_type=jnp.float32).reshape(
        length, shared_count, HEAD_DIM
    )
    key_heads = rotary(key_heads, cosine_table, sine_table).astype(jnp.bfloat16)
    value_heads = (
        jnp.dot(normed, value_matrix, preferred_element_type=jnp.float32)
        .astype(jnp.bfloat16)
        .reshape(length, shared_count, HEAD_DIM)
    )
    scores = jnp.einsum(
        "qgrd,kgd->grqk", queries.astype(jnp.float32), key_heads.astype(jnp.float32)
    ) * HEAD_DIM ** (-0.5)
    row_ids = lax.broadcasted_iota(jnp.int32, (length, length), 0)
    col_ids = lax.broadcasted_iota(jnp.int32, (length, length), 1)
    scores = jnp.where(col_ids <= row_ids, scores, -1e30)
    highest = lax.stop_gradient(jnp.max(scores, -1, keepdims=True))
    exponent = jnp.exp(scores - highest)
    weights = (exponent / jnp.sum(exponent, -1, keepdims=True)).astype(jnp.bfloat16)
    context = jnp.einsum(
        "grqk,kgd->qgrd", weights.astype(jnp.float32), value_heads.astype(jnp.float32)
    )
    context = context.astype(jnp.bfloat16).reshape(length, query_count * HEAD_DIM)
    return lax.dot_general(
        context, output_matrix, (((1,), (1,)), ((), ())), preferred_element_type=jnp.float32
    )


def server_kernel(
    rows_ref, upstream_ref, gain_ref, gate_ref, up_ref, down_ref, out_ref, normed_ref, total_ref
):
    step = pl.program_id(0)

    def inverse_rms(rows_float):
        return lax.rsqrt(jnp.mean(rows_float * rows_float, -1, keepdims=True) + 1e-05)

    @pl.when(step == 0)
    def _():
        rows_float = rows_ref[...].astype(F32)
        normed_ref[...] = (
            rows_float * inverse_rms(rows_float) * gain_ref[...].astype(F32)
        ).astype(BF16)

    gate, up = gate_ref[...], up_ref[...]
    crossed = (((1,), (1,)), ((), ()))
    gate_value = jnp.dot(normed_ref[...], gate, preferred_element_type=F32)
    up_value = jnp.dot(normed_ref[...], up, preferred_element_type=F32)
    pulled = lax.dot_general(
        upstream_ref[...], down_ref[...], crossed, preferred_element_type=F32
    )
    sigmoid_gate = jax.nn.sigmoid(gate_value)
    gate_grad = (
        pulled * up_value * sigmoid_gate * (1.0 + gate_value * (1.0 - sigmoid_gate))
    ).astype(BF16)
    up_grad = (pulled * gate_value * sigmoid_gate).astype(BF16)
    normed_grad = lax.dot_general(
        gate_grad, gate, crossed, preferred_element_type=F32
    ) + lax.dot_general(up_grad, up, crossed, preferred_element_type=F32)

    @pl.when(step == 0)
    def _():
        total_ref[...] = normed_grad

    @pl.when(step > 0)
    def _():
        total_ref[...] += normed_grad

    @pl.when(step == pl.num_programs(0) - 1)
    def _():
        rows_float = rows_ref[...].astype(F32)
        inv_rms = inverse_rms(rows_float)
        weighted = total_ref[...] * gain_ref[...].astype(F32)
        out_ref[...] = (
            inv_rms * weighted
            - rows_float * inv_rms**3 * jnp.mean(weighted * rows_float, -1, keepdims=True)
        ).astype(BF16)


def server_pull(rows_in, upstream_rows, gain, gate_matrix, up_matrix, down_matrix):
    length, breadth = rows_in.shape
    hidden = gate_matrix.shape[1]
    block = next(b for b in (256, 128, hidden) if hidden % b == 0)
    whole = pl.BlockSpec((length, breadth), lambda i: (0, 0))
    tall = pl.BlockSpec((breadth, block), lambda i: (0, i))
    return pl.pallas_call(
        server_kernel,
        grid=(hidden // block,),
        out_shape=jax.ShapeDtypeStruct((length, breadth), BF16),
        in_specs=[
            whole,
            whole,
            pl.BlockSpec((1, breadth), lambda i: (0, 0)),
            tall,
            tall,
            pl.BlockSpec((block, breadth), lambda i: (i, 0)),
        ],
        out_specs=whole,
        scratch_shapes=[pltpu.VMEM((length, breadth), BF16), pltpu.VMEM((length, breadth), F32)],
        compiler_params=pltpu.CompilerParams(vmem_limit_bytes=48 * 2**20),
        name="server_pull",
    )(rows_in, upstream_rows, gain[None], gate_matrix, up_matrix, down_matrix)


def greet(others):
    barrier = pltpu.get_barrier_semaphore()
    for other in others:
        pl.semaphore_signal(barrier, inc=1, device_id=other, device_id_type=MESH)
    pl.semaphore_wait(barrier, len(others))


def send(source, target, send_sem, recv_sem, device):
    copy = pltpu.make_async_remote_copy(
        src_ref=source,
        dst_ref=target,
        send_sem=send_sem,
        recv_sem=recv_sem,
        device_id=device,
        device_id_type=MESH,
    )
    copy.start()
    return copy


def place():
    tensor_at = lax.axis_index("tensor")
    return tensor_at // CORES, lax.rem(tensor_at, CORES)


def turned(index, step, count):
    return lax.rem(index + step, count)


def columns_of(chip, core, width):
    return pl.ds(pl.multiple_of((chip * CORES + core) * width, width), width)


def partners(chips, client_count, group_count):
    chip, core = place()
    client, group = lax.axis_index("client"), lax.axis_index("sdata")
    others = [{"tensor": chip * CORES + 1 - core}]
    others += [{"tensor": turned(chip, k, chips) * CORES + core} for k in range(1, chips)]
    others += [{"client": turned(client, k, client_count)} for k in range(1, client_count)]
    others += [{"sdata": turned(group, k, group_count)} for k in range(1, group_count)]
    return others


class ShareSum:
    def __init__(self, part, pair, relay, landed, sems, chunks, chips):
        self.part, self.pair, self.relay, self.landed = part, pair, relay, landed
        self.pair_send, self.pair_recv, self.chip_send, self.chip_recv = sems
        self.chips, self.width = chips, part.shape[-1] // (CORES * chips)
        self.chip, self.core = place()
        self.copies = []
        self.pair_copies = {}
        self.chip_copies = {}
        for n, q in enumerate(chunks):
            for k in list(range(1, chips)) + [0]:
                to = turned(self.chip, k, chips)
                copy = send(
                    part.at[q, :, columns_of(to, 1 - self.core, self.width)],
                    pair.at[k, q],
                    self.pair_send.at[k, n],
                    self.pair_recv.at[k, n],
                    {"tensor": self.chip * CORES + 1 - self.core},
                )
                self.pair_copies[k, n] = copy
        for n, q in enumerate(chunks):
            for k in range(1, chips):
                to = turned(self.chip, k, chips)
                self.pair_copies[k, n].wait_recv()
                relay[k, q] = (
                    part[q, :, columns_of(to, self.core, self.width)].astype(F32)
                    + pair[k, q].astype(F32)
                ).astype(BF16)
                self.chip_copies[k, n] = send(
                    relay.at[k, q],
                    landed.at[k, q],
                    self.chip_send.at[k, n],
                    self.chip_recv.at[k, n],
                    {"tensor": to * CORES + self.core},
                )

    def get(self, n, q):
        self.pair_copies[0, n].wait_recv()
        total = self.part[q, :, columns_of(self.chip, self.core, self.width)].astype(
            F32
        ) + self.pair[0, q].astype(F32)
        for k in range(1, self.chips):
            self.chip_copies[k, n].wait_recv()
            total = total + self.landed[k, q].astype(F32)
        return total

    def finish(self):
        for copy in list(self.pair_copies.values()) + list(self.chip_copies.values()):
            copy.wait_send()


class Widen:
    def __init__(self, out, sems, chips):
        self.out, self.chips = out, chips
        self.chip_send, self.chip_recv, self.pair_send, self.pair_recv = sems
        self.chip, self.core = place()
        self.width = out.shape[-1] // (CORES * chips)
        self.started, self.forwarded, self.chip_copies = [], [], {}

    def pair_copy(self, source, k, n, q):
        cols = columns_of(turned(self.chip, self.chips - k, self.chips), self.core, self.width)
        self.forwarded.append(
            send(
                source,
                self.out.at[q, :, cols],
                self.pair_send.at[k, n],
                self.pair_recv.at[k, n],
                {"tensor": self.chip * CORES + 1 - self.core},
            )
        )

    def start(self, source, n, q):
        cols = columns_of(self.chip, self.core, self.width)
        for k in range(1, self.chips):
            self.chip_copies[k, n] = send(
                source,
                self.out.at[q, :, cols],
                self.chip_send.at[k, n],
                self.chip_recv.at[k, n],
                {"tensor": turned(self.chip, k, self.chips) * CORES + self.core},
            )
        self.pair_copy(source, 0, n, q)
        self.out[q, :, cols] = source[...]

    def forward(self, n, q):
        for k in range(1, self.chips):
            self.chip_copies[k, n].wait_recv()
            cols = columns_of(turned(self.chip, self.chips - k, self.chips), self.core, self.width)
            self.pair_copy(self.out.at[q, :, cols], k, n, q)

    def finish(self):
        for copy in self.forwarded:
            copy.wait_recv()
        for copy in self.forwarded + list(self.chip_copies.values()):
            copy.wait_send()


def out_kernel(
    chips, client_count, group_count,
    order, part, inputs, upstream,
    cut_out, up_out, up_own,
    pair, relay, landed, cut_from, cut_at, up_at, cut_put, up_put, cut_own,
    tp_sems, z_sems, y_sems, wide_sems,
):
    client, group = lax.axis_index("client"), lax.axis_index("sdata")
    chip, core = place()
    share = client_count // group_count
    width = part.shape[-1] // (CORES * chips)
    cols = columns_of(chip, core, width)
    greet(partners(chips, client_count, group_count))
    steps = list(range(1, client_count)) + [0]
    targets = [turned(client, k, client_count) for k in steps]
    up_z = []
    sums = ShareSum(part, pair, relay, landed, [tp_sems.at[i] for i in range(4)], targets, chips)
    for k in range(1, client_count):
        to = turned(client, k, client_count)
        up_z.append(
            send(
                upstream.at[to, :, cols], up_at.at[client],
                z_sems.at[0, k], z_sems.at[1, k], {"client": to},
            )
        )
    up_at[client] = upstream[client, :, cols]
    cut_z = []
    for n, (k, to) in enumerate(zip(steps, targets)):
        block = (sums.get(n, to) + inputs[to, :, cols].astype(F32)).astype(BF16)
        if k == 0:
            cut_at[client] = block
        else:
            cut_from[k] = block
            cut_z.append(
                send(
                    cut_from.at[k], cut_at.at[client],
                    z_sems.at[2, k], z_sems.at[3, k], {"client": to},
                )
            )
    widens = [
        Widen(up_out, [wide_sems.at[i] for i in range(4)], chips),
        Widen(cut_out, [wide_sems.at[i] for i in range(4, 8)], chips),
    ]
    rounds = []
    for which, (z_copies, at, put, own) in enumerate(
        ((up_z, up_at, up_put, up_own), (cut_z, cut_at, cut_put, cut_own))
    ):
        for copy in z_copies:
            copy.wait_recv()
        y_copies = []
        for d in range(1, group_count):
            to = turned(group, d, group_count)
            for i in range(share):
                put[d, i] = at[order[to * share + i]]
                y_copies.append(
                    (
                        send(
                            put.at[d, i], own.at[group * share + i],
                            y_sems.at[2 * which, d, i], y_sems.at[2 * which + 1, d, i],
                            {"sdata": to},
                        ),
                        turned(group, group_count - d, group_count) * share + i,
                    )
                )
        n = 0
        for i in range(share):
            q = group * share + i
            own[q] = at[order[group * share + i]]
            widens[which].start(own.at[q], n, q)
            rounds.append((which, n, q))
            n += 1
        for copy, q in y_copies:
            copy.wait_recv()
            widens[which].start(own.at[q], n, q)
            rounds.append((which, n, q))
            n += 1
        for copy, q in y_copies:
            copy.wait_send()
    for which, n, q in rounds:
        widens[which].forward(n, q)
    for widen in widens:
        widen.finish()
    sums.finish()
    for copy in up_z + cut_z:
        copy.wait_send()


def back_kernel(
    chips, client_count, group_count,
    inverse, part, up_own,
    grad_out,
    pair, relay, landed, y_from, y_at, z_from, own,
    tp_sems, y_sems, z_sems, wide_sems,
):
    client, group = lax.axis_index("client"), lax.axis_index("sdata")
    share = client_count // group_count
    greet(partners(chips, client_count, group_count))
    steps = [(d, i) for d in list(range(1, group_count)) + [0] for i in range(share)]
    chunks = [turned(group, d, group_count) * share + i for d, i in steps]
    sums = ShareSum(part, pair, relay, landed, [tp_sems.at[i] for i in range(4)], chunks, chips)
    y_copies = []
    for n, ((d, i), q) in enumerate(zip(steps, chunks)):
        block = (sums.get(n, q) + up_own[q].astype(F32)).astype(BF16)
        if d == 0:
            y_at[group * share + i] = block
        else:
            y_from[d, i] = block
            y_copies.append(
                send(
                    y_from.at[d, i], y_at.at[group * share + i],
                    y_sems.at[0, d, i], y_sems.at[1, d, i],
                    {"sdata": turned(group, d, group_count)},
                )
            )
    for copy in y_copies:
        copy.wait_recv()
    widen = Widen(grad_out, [wide_sems.at[i] for i in range(4)], chips)
    z_copies = []
    for k in list(range(1, client_count)):
        to = turned(client, k, client_count)
        z_from[k] = y_at[inverse[to]]
        z_copies.append(
            send(
                z_from.at[k], own.at[client], z_sems.at[0, k], z_sems.at[1, k], {"client": to}
            )
        )
    own[client] = y_at[inverse[client]]
    widen.start(own.at[client], 0, client)
    for k, copy in enumerate(z_copies, 1):
        copy.wait_recv()
        source = turned(client, client_count - k, client_count)
        widen.start(own.at[source], k, source)
    for k in range(client_count):
        widen.forward(k, turned(client, client_count - k, client_count))
    widen.finish()
    sums.finish()
    for copy in y_copies + z_copies:
        copy.wait_send()


def average_kernel(client_count, group_count, count, *refs):
    early, grads, outs = refs[0], refs[1 : count + 1], refs[count + 1 : 2 * count + 1]
    refs = refs[1:]
    y_at, z_from, z_at = (refs[(2 + i) * count : (3 + i) * count] for i in range(3))
    y_sems, z_sems = refs[5 * count :]
    client, group = lax.axis_index("client"), lax.axis_index("sdata")
    others = [{"client": turned(client, k, client_count)} for k in range(1, client_count)]
    others += [{"sdata": turned(group, k, group_count)} for k in range(1, group_count)]
    greet(others)
    middle = client_count // 2
    steps = [(middle + k) % client_count for k in range(client_count)]
    steps = [k for k in steps if k != 0] + [0]
    y_copies = {}
    for k in steps:
        to = turned(client, k, client_count)
        for a in range(1, count):
            for d in range(1, group_count):
                y_copies[k, a, d] = send(
                    grads[a].at[to, turned(group, d, group_count)], y_at[a].at[d, to],
                    y_sems.at[0, a, d, k], y_sems.at[1, a, d, k],
                    {"sdata": turned(group, d, group_count)},
                )
    z_copies = []
    rows = outs[0].shape[0]
    block = next(b for b in (64, 32, 16, rows) if rows % b == 0)
    for k, a in [(k, 0) for k in steps] + [(k, a) for k in steps for a in range(1, count)]:
            to = turned(client, k, client_count)
            for d in range(1, group_count if a else 1):
                y_copies[k, a, d].wait_recv()
            for r in range(0, rows, block):
                at = pl.ds(r, block)
                total = grads[a][to, group, at, :].astype(F32)
                for d in range(1, group_count):
                    other = y_at[a][d, to, at, :] if a else early[d - 1, to, at, :]
                    total = total + other.astype(F32)
                z_from[a][k, at, :] = total.astype(BF16)
            if k != 0:
                z_copies.append(
                    send(
                        z_from[a].at[k], z_at[a].at[k],
                        z_sems.at[0, a, k], z_sems.at[1, a, k], {"client": to},
                    )
                )
    for copy in z_copies:
        copy.wait_recv()
    for a in range(count):
        for r in range(0, rows, block):
            at = pl.ds(r, block)
            total = z_from[a][0, at, :].astype(F32)
            for k in range(1, client_count):
                total = total + z_at[a][k, at, :].astype(F32)
            outs[a][at, :] = (total * (1.0 / client_count)).astype(BF16)
    for copy in list(y_copies.values()) + z_copies:
        copy.wait_send()


VMEM_SPEC = pl.BlockSpec(memory_space=pltpu.VMEM)
SMEM_SPEC = pl.BlockSpec(memory_space=pltpu.SMEM)


def params(number):
    return pltpu.CompilerParams(
        collective_id=number, has_side_effects=True, vmem_limit_bytes=48 * 2**20
    )


def axis_counts():
    return lax.axis_size("tensor") // CORES, lax.axis_size("client"), lax.axis_size("sdata")


def relay_out(order, attended, rows_in, upstream):
    chips, client_count, group_count = axis_counts()
    length, breadth = rows_in.shape
    chunk, width = length // client_count, breadth // (CORES * chips)
    share = client_count // group_count
    full = (client_count, chunk, breadth)
    own = (client_count, chunk, width)
    dma = pltpu.SemaphoreType.DMA
    vmem = lambda shape: pltpu.VMEM(shape, BF16)
    cut, up, up_own = pl.pallas_call(
        partial(out_kernel, chips, client_count, group_count),
        out_shape=(
            jax.ShapeDtypeStruct(full, BF16),
            jax.ShapeDtypeStruct(full, BF16),
            jax.ShapeDtypeStruct(own, BF16),
        ),
        in_specs=[SMEM_SPEC, VMEM_SPEC, VMEM_SPEC, VMEM_SPEC],
        out_specs=(VMEM_SPEC,) * 3,
        scratch_shapes=[
            vmem((chips,) + own), vmem((chips,) + own), vmem((chips,) + own),
            vmem(own), vmem(own), vmem(own),
            vmem((group_count, share, chunk, width)), vmem((group_count, share, chunk, width)),
            vmem(own),
            dma((4, chips, client_count)), dma((4, client_count)),
            dma((4, group_count, share)), dma((8, chips, client_count)),
        ],
        compiler_params=params(1),
        name="relay_out",
    )(order, attended.reshape(full), rows_in.reshape(full), upstream.reshape(full))
    return cut.reshape(length, breadth), up.reshape(length, breadth), up_own


def relay_back(inverse, pulled, up_own):
    chips, client_count, group_count = axis_counts()
    length, breadth = pulled.shape
    chunk, width = length // client_count, breadth // (CORES * chips)
    share = client_count // group_count
    full = (client_count, chunk, breadth)
    own = (client_count, chunk, width)
    dma = pltpu.SemaphoreType.DMA
    vmem = lambda shape: pltpu.VMEM(shape, BF16)
    grad = pl.pallas_call(
        partial(back_kernel, chips, client_count, group_count),
        out_shape=jax.ShapeDtypeStruct(full, BF16),
        in_specs=[SMEM_SPEC, VMEM_SPEC, VMEM_SPEC],
        out_specs=VMEM_SPEC,
        scratch_shapes=[
            vmem((chips,) + own), vmem((chips,) + own), vmem((chips,) + own),
            vmem((group_count, share, chunk, width)), vmem(own), vmem(own), vmem(own),
            dma((4, chips, client_count)), dma((2, group_count, share)),
            dma((2, client_count)), dma((4, chips, client_count)),
        ],
        compiler_params=params(2),
        name="relay_back",
    )(inverse, pulled.reshape(full), up_own)
    return grad.reshape(length, breadth)


def send_early(grad):
    unused, client_count, group_count = axis_counts()
    group = lax.axis_index("sdata")
    blocks = grad.reshape(client_count, group_count, -1, grad.shape[1])
    arrived = []
    for d in range(1, group_count):
        block = lax.dynamic_index_in_dim(blocks, turned(group, d, group_count), 1, False)
        ring = [(g, (g + d) % group_count) for g in range(group_count)]
        arrived.append(lax.ppermute(block, "sdata", ring))
    return jnp.stack(arrived)


def average(early, grads):
    unused, client_count, group_count = axis_counts()
    count = len(grads)
    rows = grads[0].shape[0] // (client_count * group_count)
    widths = [grad.shape[1] for grad in grads]
    dma = pltpu.SemaphoreType.DMA
    return pl.pallas_call(
        partial(average_kernel, client_count, group_count, count),
        out_shape=tuple(jax.ShapeDtypeStruct((rows, width), BF16) for width in widths),
        in_specs=[VMEM_SPEC] * (count + 1),
        out_specs=(VMEM_SPEC,) * count,
        scratch_shapes=[
            pltpu.VMEM((group_count, client_count, rows, w) if n else (16, 128), BF16)
            for n, w in enumerate(widths)
        ]
        + [pltpu.VMEM((client_count, rows, w), BF16) for w in widths]
        + [pltpu.VMEM((client_count, rows, w), BF16) for w in widths]
        + [dma((2, count, group_count, client_count)), dma((2, count, client_count))],
        compiler_params=params(3),
        name="average",
    )(early, *[grad.reshape(client_count, group_count, rows, grad.shape[1]) for grad in grads])


def local(
    client_input,
    client_gain,
    query_weight,
    key_weight,
    client_value_weight,
    output_weight,
    server_gain,
    server_gate,
    server_up,
    server_down,
    upstream,
    assignment,
):
    client_count = lax.axis_size("client")
    normed = normalize(client_input, client_gain[0])
    attended, pullback = jax.vjp(
        partial(attention_part, normed),
        query_weight[0],
        key_weight[0],
        client_value_weight[0],
        output_weight[0],
    )
    ids = jnp.arange(client_count).astype(jnp.int32)
    ahead = (assignment[None, :] < assignment[:, None]) | (
        (assignment[None, :] == assignment[:, None]) & (ids[None, :] < ids[:, None])
    )
    inverse = jnp.sum(ahead.astype(jnp.int32), 1)
    group_order = jnp.sum(jnp.where(inverse[None, :] == ids[:, None], ids[None, :], 0), 1)
    cut_rows, up_rows, up_own = relay_out(
        group_order, attended.astype(BF16), client_input, upstream
    )
    pulled = server_pull(
        cut_rows, up_rows, server_gain[0], server_gate[0], server_up[0], server_down[0]
    )
    arriving_grad = relay_back(inverse, pulled, up_own)
    query_grad, key_grad, value_grad, output_grad = pullback(arriving_grad.astype(jnp.float32))
    output_update, query_update, key_update, value_update = average(
        send_early(output_grad), [output_grad, query_grad, key_grad, value_grad]
    )
    return (query_update, key_update, value_update, output_update)


def solution(mesh):
    placed = (
        P(("client", "sdata"), None),
        P("client", None),
        P("client", None, "tensor"),
        P("client", None, "tensor"),
        P("client", None, "tensor"),
        P("client", None, "tensor"),
        P("sdata", None),
        P("sdata", None, "tensor"),
        P("sdata", None, "tensor"),
        P("sdata", "tensor", None),
        P(("client", "sdata"), None),
        P(),
    )
    return jax.shard_map(
        local,
        mesh=mesh,
        in_specs=placed,
        out_specs=(
            P(("client", "sdata"), "tensor"),
            P(("client", "sdata"), "tensor"),
            P(("client", "sdata"), "tensor"),
            P(("client", "sdata"), "tensor"),
        ),
        check_vma=False,
    )
```
